32 devices in a mesh: zero: 4 (over y, x), width: 2 (over core), site: 4 (over z).
Axes of the slice: x: 2, y: 2, z: 4, core: 2. Of those that a mesh axis runs over, the one named last changes fastest.
Arguments:
- train_query: bfloat16 [28672, 7168], P(('site', 'zero'), 'width'), parts along dimension 0, may hold values from -0.09375 to 0.09375
- low_query: bfloat16 [28672, 64], P(('site', 'zero')), parts along dimension 0, may hold values from -0.0625 to 0.0625
- high_query: bfloat16 [256, 7168], P('site', 'width'), parts along dimension 0, may hold values from -0.75 to 0.75
- train_key: bfloat16 [28672, 7168], P(('site', 'zero'), 'width'), parts along dimension 0, may hold values from -0.09375 to 0.09375
- low_key: bfloat16 [28672, 64], P(('site', 'zero')), parts along dimension 0, may hold values from -0.0625 to 0.0625
- high_key: bfloat16 [256, 7168], P('site', 'width'), parts along dimension 0, may hold values from -0.75 to 0.75
- train_value: bfloat16 [28672, 7168], P(('site', 'zero'), 'width'), parts along dimension 0, may hold values from -0.09375 to 0.09375
- low_value: bfloat16 [28672, 64], P(('site', 'zero')), parts along dimension 0, may hold values from -0.0625 to 0.0625
- high_value: bfloat16 [256, 7168], P('site', 'width'), parts along dimension 0, may hold values from -0.75 to 0.75
- norm_train: float32 [28672], P(('site', 'zero', 'width')), parts along dimension 0, may hold values from 0.25 to 1.75
- norm_step: float32 [28672], P(('site', 'zero', 'width')), parts along dimension 0, may hold values from -0.3 to 0.3
Outputs:
- final_query: bfloat16 [28672, 7168], P('site', ('width', 'zero')), parts along dimension 0
- final_key: bfloat16 [28672, 7168], P('site', ('width', 'zero')), parts along dimension 0
- final_value: bfloat16 [28672, 7168], P('site', ('width', 'zero')), parts along dimension 0
- scale_query: float32 [28672], P(('site', 'width', 'zero')), parts along dimension 0
- scale_key: float32 [28672], P(('site', 'width', 'zero')), parts along dimension 0
- scale_value: float32 [28672], P(('site', 'width', 'zero')), parts along dimension 0
- serve_norm: bfloat16 [28672], P('site'), parts along dimension 0
The draws below stay inside these ranges and needn't reach their ends.
There are 4 independent parts, one for each index of `site`. The reference program is written for one: setup_inputs(seed, part) draws one part's arguments, and reference() takes and returns one part's arrays. A program takes and returns all parts, laid end to end along the dimension named above; each array names one. Nothing has to cross between parts.
All inputs are finite; a program needn't handle non-finite values. Where the reference program divides by a largest or mean magnitude, that divisor is 1e-20 or more.
Results may differ from the reference program's by a relative error of at most 0.01.
Values may be sent and summed in bfloat16 or wider, within the bound.
A program may use at most 256 MiB of HBM per device.

```python
import jax
import jax.numpy as jnp

D_MODEL = 7168
Q_DIM = 7168
KV_DIM = 7168
RANK = 64


def with_spikes(values, own_key, source, target, shards_of, factor):
    owner, partner = [(jnp.arange(values.shape[position]) // (values.shape[position] // shards_of)).reshape([-1 if axis == position else 1 for axis in range(values.ndim)]) for position in (source, target)]
    chosen = jax.random.permutation(own_key, shards_of)[partner]
    strong = (owner == chosen) | (owner == (partner + shards_of // 2) % shards_of)
    return jnp.where(strong, factor * values, values)


def block_levels(rng, extent, pieces, smallest, high):
    loudness = 1.0
    for position, parts in pieces:
        heights = jax.random.uniform(jax.random.fold_in(jax.random.fold_in(rng, 6), position), (parts,), jnp.float32, smallest / len(pieces), high / len(pieces))
        loudness = loudness * jnp.repeat(jnp.exp(heights), extent[position] // parts).reshape((-1,) + (1,) * (len(extent) - 1 - position))
    return loudness


def scatter_about(key, extent, scale, most, pieces=(), dtype=jnp.bfloat16):
    loudness = block_levels(key, extent, pieces, -0.22, 0.18) if pieces else 1.0
    values = jax.random.normal(key, extent, jnp.float32) * scale * loudness
    return jnp.minimum(jnp.maximum(values, -most), most).astype(dtype)


def gaussian_with(own_key, shape, width, reach, shards, heavy, held_as=jnp.bfloat16):
    array = width * jax.random.normal(own_key, shape, jnp.float32)
    if shards:
        array = array * block_levels(own_key, shape, shards, -0.22, 0.18)
    return jnp.clip(with_spikes(array, jax.random.fold_in(own_key, 3), *heavy), -reach, reach).astype(held_as)


def setup_inputs(seed: int = 0, part: int = 0) -> dict:
    key_list = jax.random.split(jax.random.key(seed), 12)
    own_keys = jax.random.split(jax.random.fold_in(key_list[11], part), 12)
    train_query = gaussian_with(own_keys[0], (D_MODEL, Q_DIM), D_MODEL ** -0.5, 0.09375, ((0, 4), (1, 2)), (0, 1, 4, 2.0))
    low_query = scatter_about(own_keys[1], (D_MODEL, RANK), D_MODEL ** -0.5, 0.0625, ((0, 4),))
    high_query = scatter_about(own_keys[2], (RANK, Q_DIM), RANK ** -0.5, 0.75, ((1, 2),))
    train_key = gaussian_with(own_keys[3], (D_MODEL, KV_DIM), D_MODEL ** -0.5, 0.09375, ((0, 4), (1, 2)), (0, 1, 4, 2.0))
    low_key = scatter_about(own_keys[4], (D_MODEL, RANK), D_MODEL ** -0.5, 0.0625, ((0, 4),))
    high_key = scatter_about(own_keys[5], (RANK, KV_DIM), RANK ** -0.5, 0.75, ((1, 2),))
    train_value = gaussian_with(own_keys[6], (D_MODEL, KV_DIM), D_MODEL ** -0.5, 0.09375, ((0, 4), (1, 2)), (0, 1, 4, 2.0))
    low_value = scatter_about(own_keys[7], (D_MODEL, RANK), D_MODEL ** -0.5, 0.0625, ((0, 4),))
    high_value = scatter_about(own_keys[8], (RANK, KV_DIM), RANK ** -0.5, 0.75, ((1, 2),))
    norm_train = jnp.clip(1.0 + 0.15 * jax.random.normal(own_keys[9], (D_MODEL,), jnp.float32), 0.25, 1.75)
    norm_step = jnp.clip(jax.random.uniform(own_keys[10], (D_MODEL,), jnp.float32, -0.3, 0.3) * block_levels(own_keys[10], (D_MODEL,), ((0, 8),), -0.4, 0.0), -0.3, 0.3)
    return dict(train_query=train_query, low_query=low_query, high_query=high_query, train_key=train_key, low_key=low_key, high_key=high_key, train_value=train_value, low_value=low_value, high_value=high_value, norm_train=norm_train, norm_step=norm_step)


mix_rate = 1.0


def reference(train_query, low_query, high_query, train_key, low_key, high_key, train_value, low_value, high_value, norm_train, norm_step):
    result_query = train_query.astype(jnp.float32) + mix_rate * jnp.dot(low_query, high_query, preferred_element_type=jnp.float32)
    result_key = train_key.astype(jnp.float32) + mix_rate * jnp.dot(low_key, high_key, preferred_element_type=jnp.float32)
    result_value = train_value.astype(jnp.float32) + mix_rate * jnp.dot(low_value, high_value, preferred_element_type=jnp.float32)
    scale_query = jnp.sum(jnp.abs(result_query), axis=0) / D_MODEL
    final_query = (result_query / scale_query).astype(jnp.bfloat16)
    scale_key = jnp.sum(jnp.abs(result_key), axis=0) / D_MODEL
    final_key = (result_key / scale_key).astype(jnp.bfloat16)
    scale_value = jnp.sum(jnp.abs(result_value), axis=0) / D_MODEL
    final_value = (result_value / scale_value).astype(jnp.bfloat16)
    serve_norm = (norm_train + norm_step).astype(jnp.bfloat16)
    return final_query, final_key, final_value, scale_query, scale_key, scale_value, serve_norm
```

```python
import functools

import jax
import jax.numpy as jnp
from jax import lax
from jax.experimental import pallas as pl
from jax.experimental.pallas import tpu as pltpu
from jax.sharding import PartitionSpec as P


mix_rate = 1.0
LANES = 128
CUTS = ((1,), (), (-1,))


def merged(train, low, high):
    product = jnp.dot(low, high, preferred_element_type=jnp.float32)
    return (train.astype(jnp.float32) + mix_rate * product).astype(jnp.bfloat16)


def finish_body(peers, tiles, step, offset, extra, *refs):
    blocks, rest = refs[:peers], refs[peers + extra :]
    out_ref, scale_ref, held, in_sem, out_sem = rest
    rows, columns = blocks[0].shape
    tile = rows // tiles
    me = lax.axis_index("zero")

    def fetch(m, t):
        span = pl.ds(t * tile, tile)
        return pltpu.make_async_copy(blocks[m].at[span], held.at[m, span], in_sem.at[m, t])

    def put(m, t):
        span = pl.ds(t * tile, tile)
        place = pl.multiple_of((me ^ m) * rows + t * tile, 16)
        target = out_ref.at[pl.ds(place, tile), pl.ds(offset, columns)]
        return pltpu.make_async_copy(held.at[m, span], target, out_sem.at[m, t])

    for m in range(peers):
        for t in range(tiles):
            fetch(m, t).start()
    total = jnp.zeros((8, columns), jnp.float32)
    for m in range(peers):
        for t in range(tiles):
            fetch(m, t).wait()

            def add(i, acc, m=m, t=t):
                base = pl.multiple_of(t * tile + i * step, step)
                size = jnp.abs(held[m, pl.ds(base, step), :].astype(jnp.float32))
                while size.shape[0] > 8:
                    half = size.shape[0] // 2
                    size = size[:half] + size[half:]
                return acc + size

            total = lax.fori_loop(0, tile // step, add, total)
    scale = jnp.sum(total, axis=0, keepdims=True) / (rows * peers)
    scale_ref[...] = scale
    inverse = 1.0 / scale
    for m in range(peers):
        for t in range(tiles):

            def divide(i, carry, m=m, t=t):
                base = pl.multiple_of(t * tile + i * step, step)
                span = pl.ds(base, step)
                held[m, span, :] = (held[m, span, :].astype(jnp.float32) * inverse).astype(
                    jnp.bfloat16
                )
                return carry

            lax.fori_loop(0, tile // step, divide, 0)
            put(m, t).start()
    for m in range(peers):
        for t in range(tiles):
            put(m, t).wait()


def finish(blocks, previous, after, offset, width):
    peers = len(blocks)
    rows, columns = blocks[0].shape
    tiles = 7 if rows % (7 * 32) == 0 else 1
    tile = rows // tiles
    step = max(s for s in (16, 32, 64, 128, 256) if tile % s == 0 and (s == 16 or s * columns <= 1 << 16))
    aliased = previous is not None
    operands = list(blocks) + ([previous] if aliased else []) + ([] if after is None else [after])
    size = 2 * rows * peers * columns
    return pl.pallas_call(
        functools.partial(finish_body, peers, tiles, step, offset, len(operands) - peers),
        out_shape=(
            jax.ShapeDtypeStruct((rows * peers, width), jnp.bfloat16),
            jax.ShapeDtypeStruct((1, columns), jnp.float32),
        ),
        in_specs=[pl.BlockSpec(memory_space=pl.ANY)] * len(operands),
        out_specs=(pl.BlockSpec(memory_space=pl.ANY), pl.BlockSpec(memory_space=pltpu.VMEM)),
        scratch_shapes=[
            pltpu.VMEM((peers, rows, columns), jnp.bfloat16),
            pltpu.SemaphoreType.DMA((peers, tiles)),
            pltpu.SemaphoreType.DMA((peers, tiles)),
        ],
        input_output_aliases={peers: 0} if aliased else {},
        compiler_params=pltpu.CompilerParams(vmem_limit_bytes=size + (4 << 20)),
        cost_estimate=pl.CostEstimate(
            flops=4 * size, bytes_accessed=2 * size, transcendentals=0
        ),
        name="finish",
    )(*operands)


def pairs(n, m):
    return [(i, i ^ m) for i in range(n)]


def cuts_of(width, inner):
    lanes = width // LANES
    return [0] + [cut % lanes * LANES for cut in inner if lanes > 1] + [width]


def project_all(triples, gain, n, w):
    me, core = lax.axis_index("zero"), lax.axis_index("width")

    def send(block, m):
        return lax.ppermute(block, "zero", pairs(n, m))

    order = sorted(range(1, n), key=lambda m: (-bin(m).count("1"), m)) + [0]
    chunks, last, gains, step = [], None, None, 0
    for index, (train, low, high) in enumerate(triples):
        width = train.shape[1] // n
        cuts = cuts_of(width, CUTS[index])
        for begin, end in zip(cuts[:-1], cuts[1:]):
            blocks = {}
            for m in order:
                if last is not None:
                    low, last = lax.optimization_barrier((low, last))
                at = (me ^ m) * width + begin
                last = merged(
                    lax.dynamic_slice_in_dim(train, at, end - begin, axis=1),
                    low,
                    lax.dynamic_slice_in_dim(high, at, end - begin, axis=1),
                )
                blocks[m] = send(last, m) if m else last
                step += 1
            chunks.append((index, begin, width, [blocks[m] for m in range(n)]))
        if gains is None:
            gain, last = lax.optimization_barrier((gain, last))
            other = lax.ppermute(gain, "width", pairs(w, 1))
            both = jnp.where(core == 0, jnp.stack([gain, other]), jnp.stack([other, gain]))
            both, last = lax.optimization_barrier((both, last))
            gains = [send(both, m) if m else both for m in range(n)]
    outs, scales, after = [None] * len(triples), [[] for _ in triples], None
    for index, begin, width, blocks in chunks:
        outs[index], after = finish(blocks, outs[index], after, begin, width)
        scales[index].append(after)
        if index == 1 and begin == 0:
            gains, after = lax.optimization_barrier((gains, after))
            gain = jnp.stack(gains)[jnp.arange(n) ^ me].reshape(-1)
    return outs, [jnp.concatenate(s, axis=1).reshape(-1) for s in scales], gain


def project_plain(train, low, high):
    result = lax.all_to_all(merged(train, low, high), "zero", split_axis=1, concat_axis=0, tiled=True)
    result = result.astype(jnp.float32)
    scale = jnp.sum(jnp.abs(result), axis=0) / result.shape[0]
    return (result / scale).astype(jnp.bfloat16), scale


def shards(n, w, tq, lq, hq, tk, lk, hk, tv, lv, hv, norm_train, norm_step):
    width = tq.shape[1] // n
    direct = n & (n - 1) == 0 and n <= 8 and w == 2
    direct = direct and width % LANES == 0 and tq.shape[0] % 16 == 0
    gain = (norm_train + norm_step).astype(jnp.bfloat16)
    triples = ((tq, lq, hq), (tk, lk, hk), (tv, lv, hv))
    if direct:
        outs, scales, serve_norm = project_all(triples, gain, n, w)
    else:
        outs, scales = zip(*(project_plain(*triple) for triple in triples))
        serve_norm = lax.all_gather(gain, ("zero", "width"), axis=0, tiled=True)
    return (*outs, *scales, serve_norm)


def solution(mesh):
    rows, whole, columns = P(("site", "zero"), "width"), P(("site", "zero"), None), P("site", "width")
    vector = P(("site", "zero", "width"))
    matrix_out, vector_out = P("site", ("width", "zero")), P(("site", "width", "zero"))
    n, w = mesh.shape["zero"], mesh.shape["width"]

    def body(*arrays):
        return shards(n, w, *arrays)

    return jax.shard_map(
        body,
        mesh=mesh,
        in_specs=(rows, whole, columns) * 3 + (vector, vector),
        out_specs=(matrix_out,) * 3 + (vector_out,) * 3 + (P("site"),),
        check_vma=False,
    )
```
